32 devices in a mesh: gx: 4 (over z), gy: 8 (over y, x, core).
Axes of the slice: x: 2, y: 2, z: 4, core: 2. Of those that a mesh axis runs over, the one named last changes fastest.
Arguments:
- field: float32 [256, 3072], P('gx', 'gy'), may hold values from -9 to 9
- decay_x: float32 [256, 8], P('gx'), may hold values from 0.15 to 0.99999
- decay_y: float32 [384, 8], P('gy'), may hold values from 0.15 to 0.99999
Outputs:
- smoothed: float32 [256, 3072], P('gx', 'gy')
The draws below stay inside these ranges and needn't reach their ends.
All inputs are finite; a program needn't handle non-finite values.
Results may differ from the reference program's by a relative error of at most 0.0003.
Values sent between devices are 32-bit elements; how exact they have to be, the bound alone decides.
A program may use at most 64 MiB of HBM per device.

```python
import math
import jax
import jax.numpy as jnp
from jax import lax

CX = 64
CY = 48
VERTICAL_LAYERS = 8
PASSES = 1
NX = 256
NY = 384


def decay_draw(key, length_scale, block):
    keys = jax.random.split(key, 4)
    lowest = 20.0
    highest = 4.0 * length_scale
    spreads = jax.random.uniform(keys[0], (VERTICAL_LAYERS,), jnp.float32)
    scale_values = lowest * (highest / lowest) ** spreads
    rough_noise = jnp.exp(jax.random.uniform(keys[1], (length_scale, VERTICAL_LAYERS), jnp.float32, math.log(0.6), math.log(1.5)))
    processor_multiplier = jnp.exp(jax.random.uniform(keys[2], (length_scale // block, VERTICAL_LAYERS), jnp.float32, math.log(0.7), math.log(1.4)))
    processor_multiplier = jnp.repeat(processor_multiplier, block, axis=0)
    probe_points = jax.random.randint(keys[3], (3, VERTICAL_LAYERS), 0, length_scale)
    grid_location = jnp.arange(length_scale)
    impulse_spike = jnp.ones((length_scale, VERTICAL_LAYERS), jnp.float32)
    for selected_index in range(3):
        impulse_spike = impulse_spike * jnp.where(grid_location[:, None] == probe_points[selected_index][None, :], 0.6, 1.0)
    decay_factors = jnp.exp(-1.0 / (scale_values[None, :] * rough_noise * processor_multiplier)) * impulse_spike
    return decay_factors.astype(jnp.float32)


def draw_decay_x(key, part):
    return decay_draw(jax.random.fold_in(key, 21), NX, CX)


def draw_decay_y(key, part):
    return decay_draw(jax.random.fold_in(key, 22), NY, CY)


def draw_field(key, part):
    keys = jax.random.split(jax.random.fold_in(key, 11), 5)
    noise = jax.random.truncated_normal(keys[0], -5.0, 5.0, (NX, NY, VERTICAL_LAYERS), jnp.float32)
    across = jnp.arange(NX, dtype=jnp.float32) / NX
    along = jnp.arange(NY, dtype=jnp.float32) / NY
    waves_x = jax.random.randint(keys[1], (3, VERTICAL_LAYERS), 1, 5).astype(jnp.float32)
    waves_y = jax.random.randint(keys[2], (3, VERTICAL_LAYERS), 1, 5).astype(jnp.float32)
    phases = jax.random.uniform(keys[3], (2, 3, VERTICAL_LAYERS), jnp.float32)
    amplitude = jax.random.uniform(keys[4], (3, VERTICAL_LAYERS), jnp.float32, -1.0, 1.0)
    smooth = jnp.zeros((NX, NY, VERTICAL_LAYERS), jnp.float32)
    for selected_index in range(3):
        first = jnp.cos(2.0 * math.pi * (waves_x[selected_index][None, :] * across[:, None] + phases[0, selected_index][None, :]))
        second = jnp.cos(2.0 * math.pi * (waves_y[selected_index][None, :] * along[:, None] + phases[1, selected_index][None, :]))
        smooth = smooth + amplitude[selected_index][None, None, :] * first[:, None, :] * second[None, :, :]
    return (noise + smooth).reshape(NX, NY * VERTICAL_LAYERS).astype(jnp.float32)


def setup_inputs(seed: int = 0) -> dict:
    arg_keys = jax.random.split(jax.random.key(seed), 4)
    field = draw_field(jax.random.fold_in(arg_keys[3], 71), 0)
    decay_x = draw_decay_x(jax.random.fold_in(arg_keys[3], 71), 0)
    decay_y = draw_decay_y(jax.random.fold_in(arg_keys[3], 71), 0)
    return dict(field=field, decay_x=decay_x, decay_y=decay_y)


def sweep(grid, decay_factors, backward):
    gains = 1.0 - decay_factors
    width = grid.shape[1]

    def advance(states, inputs):
        values, decay, gain = inputs
        first = decay * states[0] + gain * values
        second = decay * states[1] + gain * first
        third = decay * states[2] + gain * second
        fourth = decay * states[3] + gain * third
        return (first, second, third, fourth), fourth

    zero = jnp.zeros((width, VERTICAL_LAYERS), jnp.float32)
    final, outputs = lax.scan(advance, (zero, zero, zero, zero), (grid, decay_factors, gains), reverse=backward)
    return outputs


def reference(field, decay_x, decay_y):
    grid = field.reshape(NX, NY, VERTICAL_LAYERS)
    for repeat in range(PASSES):
        grid = sweep(grid, decay_x, False)
        grid = sweep(grid, decay_x, True)
        turned = jnp.transpose(grid, (1, 0, 2))
        turned = sweep(turned, decay_y, False)
        turned = sweep(turned, decay_y, True)
        grid = jnp.transpose(turned, (1, 0, 2))
    return grid.reshape(NX, NY * VERTICAL_LAYERS)
```

```python
import functools

import jax
import jax.numpy as jnp
from jax import lax
from jax.experimental import pallas as pl
from jax.experimental.pallas import tpu as pltpu
from jax.sharding import PartitionSpec as P

LANES = 128
SUB = 8
HIGHEST = lax.Precision.HIGHEST
UNROLL = 8


def iota(dimension):
    return lax.broadcasted_iota(jnp.int32, (SUB, LANES), dimension)


def rows_of(i):
    return pl.ds(pl.multiple_of(i * SUB, SUB), SUB)


def spread(row):
    return jnp.broadcast_to(row, (SUB, LANES))


def sweep(count, slots, decay, load, mid, emit):
    sub = iota(0)
    zero = jnp.zeros((SUB, LANES), jnp.float32)

    def advance(i, states, value):
        a = decay[pl.ds(i, 1), :]
        g = 1.0 - a
        result = []
        for state in states:
            value = a * state + g * value
            result.append(value)
        return tuple(result)

    def forward(i, states):
        states = advance(i, states, load(i))
        kept = states[3]
        for order in range(3):
            kept = jnp.where(sub == slots + 1 + order, states[order], kept)
        mid[rows_of(i), :] = kept
        return states

    def backward(i, states):
        states = advance(i, states, mid[rows_of(i), :])
        emit(i, states)
        return states

    def chunks(step, states, reverse):
        width = UNROLL if count % UNROLL == 0 else 1

        def chunk(j, states):
            for u in range(width):
                i = j * width + u
                states = step(count - 1 - i if reverse else i, states)
            return states

        return lax.fori_loop(0, count // width, chunk, states)

    one = jnp.where(sub > slots, 1.0, 0.0)
    first = chunks(forward, (one, zero, zero, zero), False)
    one = jnp.where(sub == slots, 1.0, 0.0)
    second = chunks(backward, (one, zero, zero, zero), True)
    return first, second


def compose(devices, mine, slots, ends, maps):
    zero = jnp.zeros((SUB, LANES), jnp.float32)
    state = [zero] * 4
    entering = []
    picked = [zero] * 4
    for p in range(devices):
        entering.append(state)
        picked = [jnp.where(mine == p, new, old) for new, old in zip(state, picked)]
        if p == devices - 1:
            break
        r = [maps(p, k)[slots + 1 : slots + 2, :] for k in range(4)]
        state = [
            ends(p, k) + sum(r[k - m] * state[m] for m in range(k + 1)) for k in range(4)
        ]
    ahead = picked
    state = [zero] * 4
    picked = [zero] * 4
    for p in range(devices - 1, -1, -1):
        picked = [jnp.where(mine == p, new, old) for new, old in zip(state, picked)]
        if p == 0:
            break
        back = [maps(p, 4 + k) for k in range(4)]
        r = [back[k][slots : slots + 1, :] for k in range(4)]
        before = entering[p]
        state = [
            ends(p, 4 + k)
            + sum(r[k - m] * state[m] for m in range(k + 1))
            + sum(back[k][slots + 4 - m : slots + 5 - m, :] * before[m] for m in range(4))
            for k in range(4)
        ]
    return ahead, picked


def kernel(
    nx, ny, cx, cy, slots,
    field, decay_x, decay_y, out,
    ax, ay, xin, mid, xout, xresp, grid, wt, yacc,
    xsend, xrecv, msend, mrecv, ysend, yrecv,
    xs, xr, ms, mr, ys, yr,
):
    levels = decay_x.shape[1]
    group = LANES // levels
    blocks = cx // SUB
    mx, my = lax.axis_index("gx"), lax.axis_index("gy")
    barrier = pltpu.get_barrier_semaphore()
    for d in range(1, nx):
        pl.semaphore_signal(barrier, inc=1, device_id=(lax.rem(mx + d, nx), my), device_id_type=pl.DeviceIdType.MESH)
    for d in range(1, ny):
        pl.semaphore_signal(barrier, inc=1, device_id=(mx, lax.rem(my + d, ny)), device_id_type=pl.DeviceIdType.MESH)

    sub, lane = iota(0), iota(1)
    lane_group = lane // levels
    tiling = jnp.where(
        lax.broadcasted_iota(jnp.int32, (levels, LANES), 1) % levels
        == lax.broadcasted_iota(jnp.int32, (levels, LANES), 0),
        1.0,
        0.0,
    )
    ax[...] = jnp.dot(decay_x[...], tiling, precision=HIGHEST, preferred_element_type=jnp.float32)
    ay[...] = jnp.dot(decay_y[...], tiling, precision=HIGHEST, preferred_element_type=jnp.float32)
    for b in range(blocks):
        for s in range(slots):
            xin[pl.ds(b * SUB * SUB + s, SUB, stride=SUB), :] = field[
                b * SUB : (b + 1) * SUB, s * LANES : (s + 1) * LANES
            ]

    def emit_x(i, states):
        xout[rows_of(i), :] = states[3]
        for order in range(3):
            xresp[order, rows_of(i), :] = states[order]

    first, second = sweep(
        cx, slots, ax, lambda i: jnp.where(sub < slots, xin[rows_of(i), :], 0.0), mid, emit_x
    )
    for k in range(4):
        xsend[k] = first[k]
        xsend[4 + k] = second[k]
        xrecv[mx, k] = first[k]
        xrecv[mx, 4 + k] = second[k]

    pl.semaphore_wait(barrier, nx + ny - 2)

    def along_x(d):
        return (lax.rem(mx + d, nx), my), lax.rem(mx + d, nx)

    def along_y(d):
        return (mx, lax.rem(my + d, ny)), lax.rem(my + d, ny)

    def copies(count, mine, along, src, dst, ssem, rsem):
        sends, receives = [], []
        for d in range(1, count):
            where, index = along(d)
            sends.append(
                pltpu.make_async_remote_copy(
                    src_ref=src, dst_ref=dst.at[mine], send_sem=ssem.at[d], recv_sem=rsem.at[mine],
                    device_id=where, device_id_type=pl.DeviceIdType.MESH,
                )
            )
            receives.append(
                pltpu.make_async_remote_copy(
                    src_ref=src, dst_ref=dst.at[index], send_sem=ssem.at[d], recv_sem=rsem.at[index],
                    device_id=where, device_id_type=pl.DeviceIdType.MESH,
                )
            )
        return sends, receives

    x_sends, x_receives = copies(nx, mx, along_x, xsend, xrecv, xs, xr)
    m_sends, m_receives = copies(ny, my, along_y, msend, mrecv, ms, mr)
    y_sends, y_receives = copies(ny, my, along_y, ysend, yrecv, ys, yr)
    for copy in x_sends:
        copy.start()

    own_level = lane % levels == sub
    yacc[...] = jnp.zeros_like(yacc)

    def impulse(i):
        return jnp.where(
            (sub < slots) & (sub * LANES + lane >= i * levels) & (sub * LANES + lane < (i + 1) * levels),
            1.0,
            0.0,
        )

    def emit_y(i, states):
        for s in range(slots):
            wt[rows_of(i), s * LANES : (s + 1) * LANES] = jnp.where(
                own_level, spread(states[3][s : s + 1, :]), 0.0
            )
        here = lane_group == lax.rem(i, group)
        chunk = i // group
        for order in range(4):
            yacc[order, chunk] = jnp.where(here, states[order], yacc[order, chunk])

    first, second = sweep(cy, slots, ay, impulse, mid, emit_y)
    for k in range(4):
        msend[k] = first[k]
        msend[4 + k] = second[k]
        mrecv[my, k] = first[k]
        mrecv[my, 4 + k] = second[k]
    for copy in m_sends:
        copy.start()
    y_ends = first + second

    for copy in x_receives:
        copy.wait_recv()
    ahead, behind = compose(nx, mx, slots, lambda p, k: xrecv[p, k], lambda p, k: xrecv[p, k])

    def tile(ref, b, s):
        return ref[pl.ds(b * SUB * SUB + s, SUB, stride=SUB), :]

    sums = []
    for b in range(blocks):
        parts = []
        g = [tile(xout, b, slots + 4 - m) for m in range(4)]
        r = [tile(xout, b, slots)] + [tile(xresp.at[2 - m], b, slots) for m in range(3)]
        for s in range(slots):
            value = tile(xout, b, s)
            for m in range(4):
                value = value + g[m] * ahead[m][s : s + 1, :] + r[m] * behind[m][s : s + 1, :]
            grid[b * SUB : (b + 1) * SUB, s * LANES : (s + 1) * LANES] = value
            parts.append(value)
        sums.append(parts)

    merge = jnp.where(
        lax.broadcasted_iota(jnp.int32, (LANES, LANES), 0) % levels
        == lax.broadcasted_iota(jnp.int32, (LANES, LANES), 1) % levels,
        1.0,
        0.0,
    )
    products = [
        sum(sums[b][s] * y_ends[k][s : s + 1, :] for s in range(slots))
        for k in range(8)
        for b in range(blocks)
    ]
    totals = jnp.dot(
        jnp.concatenate(products, axis=0), merge, precision=HIGHEST, preferred_element_type=jnp.float32
    )
    for k in range(8):
        packed = jnp.zeros((SUB, LANES), jnp.float32)
        for b in range(blocks):
            at = (k * blocks + b) * SUB
            packed = jnp.where(lane_group == b, totals[at : at + SUB, :], packed)
        ysend[k] = packed
        yrecv[my, k] = packed
    for copy in y_sends:
        copy.start()

    out[...] = lax.dot_general(
        grid[...], wt[...], (((1,), (1,)), ((), ())), precision=HIGHEST, preferred_element_type=jnp.float32
    )

    for copy in m_receives:
        copy.wait_recv()
    for copy in y_receives:
        copy.wait_recv()
    ahead, behind = compose(ny, my, slots, lambda p, k: yrecv[p, k], lambda p, k: mrecv[p, k])
    states = list(ahead) + list(behind)
    masked = [jnp.where(lane_group == b, states[m], 0.0) for m in range(8) for b in range(blocks)]
    opened = jnp.dot(
        jnp.concatenate(masked, axis=0), merge, precision=HIGHEST, preferred_element_type=jnp.float32
    )
    for s in range(slots):
        held = [yacc[order, s] for order in range(4)]
        answers = [held[3][slots + 4 - m : slots + 5 - m, :] for m in range(4)]
        answers += [held[3 - m][slots : slots + 1, :] for m in range(4)]
        for b in range(blocks):
            value = out[b * SUB : (b + 1) * SUB, s * LANES : (s + 1) * LANES]
            for m in range(8):
                at = (m * blocks + b) * SUB
                value = value + opened[at : at + SUB, :] * answers[m]
            out[b * SUB : (b + 1) * SUB, s * LANES : (s + 1) * LANES] = value
    for copy in x_sends + m_sends + y_sends:
        copy.wait_send()


def body(nx, ny, field, decay_x, decay_y):
    cx, levels = decay_x.shape
    cy = decay_y.shape[0]
    width = cy * levels
    slots = -(-width // LANES)
    padded = slots * LANES
    if padded != width:
        field = jnp.pad(field, ((0, 0), (0, padded - width)))
    longest = max(cx, cy)
    vmem = lambda *shape: pltpu.VMEM(shape, jnp.float32)
    dma = pltpu.SemaphoreType.DMA
    result = pl.pallas_call(
        functools.partial(kernel, nx, ny, cx, cy, slots),
        out_shape=jax.ShapeDtypeStruct((cx, padded), jnp.float32),
        in_specs=[pl.BlockSpec(memory_space=pltpu.VMEM)] * 3,
        out_specs=pl.BlockSpec(memory_space=pltpu.VMEM),
        scratch_shapes=[
            vmem(cx, LANES),
            vmem(cy, LANES),
            vmem(cx * SUB, LANES),
            vmem(longest * SUB, LANES),
            vmem(cx * SUB, LANES),
            vmem(3, cx * SUB, LANES),
            vmem(cx, padded),
            vmem(padded, padded),
            vmem(4, slots, SUB, LANES),
            vmem(8, SUB, LANES),
            vmem(nx, 8, SUB, LANES),
            vmem(8, SUB, LANES),
            vmem(ny, 8, SUB, LANES),
            vmem(8, SUB, LANES),
            vmem(ny, 8, SUB, LANES),
            dma((nx,)),
            dma((nx,)),
            dma((ny,)),
            dma((ny,)),
            dma((ny,)),
            dma((ny,)),
        ],
        compiler_params=pltpu.CompilerParams(collective_id=0, has_side_effects=True),
    )(field, decay_x, decay_y)
    return result[:, :width] if padded != width else result


def solution(mesh):
    placed = (P("gx", "gy"), P("gx", None), P("gy", None))
    nx, ny = mesh.shape["gx"], mesh.shape["gy"]
    return jax.shard_map(
        functools.partial(body, nx, ny), mesh=mesh, in_specs=placed, out_specs=P("gx", "gy"), check_vma=False
    )
```

```python
import functools

import jax
import jax.numpy as jnp
from jax import lax
from jax.experimental import pallas as pl
from jax.experimental.pallas import tpu as pltpu
from jax.sharding import PartitionSpec as P

LANES = 128
SUB = 8
HIGHEST = lax.Precision.HIGHEST
UNROLL = 16


def iota(dimension):
    return lax.broadcasted_iota(jnp.int32, (SUB, LANES), dimension)


def rows_of(i):
    return pl.ds(pl.multiple_of(i * SUB, SUB), SUB)


def spread(row):
    return jnp.broadcast_to(row, (SUB, LANES))


def sweep(count, slots, decay, load, mid, emit):
    sub = iota(0)
    zero = jnp.zeros((SUB, LANES), jnp.float32)

    def advance(i, states, value):
        a = decay[pl.ds(i, 1), :]
        g = 1.0 - a
        result = []
        for state in states:
            value = a * state + g * value
            result.append(value)
        return tuple(result)

    def forward(i, states):
        states = advance(i, states, load(i))
        kept = states[3]
        for order in range(3):
            kept = jnp.where(sub == slots + 1 + order, states[order], kept)
        mid[rows_of(i), :] = kept
        return states

    def backward(i, states):
        states = advance(i, states, mid[rows_of(i), :])
        emit(i, states)
        return states

    def chunks(step, states, reverse):
        width = UNROLL if count % UNROLL == 0 else 1

        def chunk(j, states):
            for u in range(width):
                i = j * width + u
                states = step(count - 1 - i if reverse else i, states)
            return states

        return lax.fori_loop(0, count // width, chunk, states)

    one = jnp.where(sub > slots, 1.0, 0.0)
    first = chunks(forward, (one, zero, zero, zero), False)
    one = jnp.where(sub == slots, 1.0, 0.0)
    second = chunks(backward, (one, zero, zero, zero), True)
    return first, second


def pack_maps(first, second, lane_group):
    packed = second[0]
    for k in range(1, 8):
        packed = jnp.where(lane_group == k, (second + first)[k], packed)
    return packed


def open_map(packed, k, lane_group, levels):
    value = jnp.where(lane_group == (k + 4) % 8, packed, 0.0)
    shift = levels
    while shift < LANES:
        value = value + pltpu.roll(value, shift, 1)
        shift *= 2
    return value


def pack_ends(ends, packed, slots):
    sub = iota(0)
    half = SUB // 2
    result = [
        jnp.where(sub < half, ends[2 * v], pltpu.roll(ends[2 * v + 1], half, 0)) for v in range(4)
    ]
    for v, at, row in map_rows(slots):
        result[v] = jnp.where(sub == at, packed[row : row + 1, :], result[v])
    return result


def map_rows(slots):
    half = SUB // 2
    last = half - 1
    return (
        (0, last, slots + 1),
        (1, last, slots),
        (2, last, slots + 2),
        (2, half + last, slots + 3),
        (3, last, slots + 4),
    )


def open_ends(vectors, k):
    vector = vectors[k // 2]
    return pltpu.roll(vector, SUB // 2, 0) if k % 2 else vector


def compose(devices, mine, slots, ends, maps):
    zero = jnp.zeros((SUB, LANES), jnp.float32)
    state = [zero] * 4
    entering = []
    picked = [zero] * 4
    for p in range(devices):
        entering.append(state)
        picked = [jnp.where(mine == p, new, old) for new, old in zip(state, picked)]
        if p == devices - 1:
            break
        r = [maps(p, k)[slots + 1 : slots + 2, :] for k in range(4)]
        state = [
            ends(p, k) + sum(r[k - m] * state[m] for m in range(k + 1)) for k in range(4)
        ]
    ahead = picked
    state = [zero] * 4
    picked = [zero] * 4
    for p in range(devices - 1, -1, -1):
        picked = [jnp.where(mine == p, new, old) for new, old in zip(state, picked)]
        if p == 0:
            break
        back = [maps(p, 4 + k) for k in range(4)]
        r = [back[k][slots : slots + 1, :] for k in range(4)]
        before = entering[p]
        state = [
            ends(p, 4 + k)
            + sum(r[k - m] * state[m] for m in range(k + 1))
            + sum(back[k][slots + 4 - m : slots + 5 - m, :] * before[m] for m in range(4))
            for k in range(4)
        ]
    return ahead, picked


def kernel(
    nx, ny, cx, cy, slots,
    field, decay_x_in, decay_y_in, out,
    decay_x, decay_y, ax, ay, xin, mid, xout, xresp, grid, wt, yacc,
    xsend, xrecv, msend, mrecv, ysend, yrecv,
    xs, xr, ms, mr, ys, yr, xs_back, xr_back, ys_back, yr_back, loaded,
):
    levels = decay_x.shape[0]
    group = LANES // levels
    blocks = cx // SUB
    mx, my = lax.axis_index("gx"), lax.axis_index("gy")
    barrier = pltpu.get_barrier_semaphore()
    for d in range(1, nx):
        pl.semaphore_signal(barrier, inc=1, device_id=(lax.rem(mx + d, nx), my), device_id_type=pl.DeviceIdType.MESH)
    for d in range(1, ny):
        pl.semaphore_signal(barrier, inc=1, device_id=(mx, lax.rem(my + d, ny)), device_id_type=pl.DeviceIdType.MESH)

    loads = [
        pltpu.make_async_copy(decay_x_in, decay_x, loaded.at[0]),
        pltpu.make_async_copy(decay_y_in, decay_y, loaded.at[1]),
    ]
    loads += [
        pltpu.make_async_copy(field.at[:, pl.ds(s * LANES, LANES)], xin.at[:, s], loaded.at[2 + s])
        for s in range(slots)
    ]
    for copy in loads:
        copy.start()

    sub, lane = iota(0), iota(1)
    lane_group = lane // levels
    tiling = jnp.where(
        lax.broadcasted_iota(jnp.int32, (levels, LANES), 1) % levels
        == lax.broadcasted_iota(jnp.int32, (levels, LANES), 0),
        1.0,
        0.0,
    )
    for copy, target, source in ((loads[0], ax, decay_x), (loads[1], ay, decay_y)):
        copy.wait()
        target[...] = lax.dot_general(
            source[...], tiling, (((0,), (0,)), ((), ())), precision=HIGHEST, preferred_element_type=jnp.float32
        )
    for copy in loads[2:]:
        copy.wait()

    def emit_x(i, states):
        xout[rows_of(i), :] = states[3]
        for order in range(3):
            xresp[order, rows_of(i), :] = states[order]

    first, second = sweep(
        cx, slots, ax, lambda i: jnp.where(sub < slots, xin[i], 0.0), mid, emit_x
    )
    packed = pack_maps(first, second, lane_group)
    for v, vector in enumerate(pack_ends(first + second, packed, slots)):
        xsend[v] = vector
        xrecv[mx, v] = vector

    pl.semaphore_wait(barrier, nx + ny - 2)

    def along_x(d):
        return (lax.rem(mx + d, nx), my), lax.rem(mx + d, nx)

    def along_y(d):
        return (mx, lax.rem(my + d, ny)), lax.rem(my + d, ny)

    def both_ways(count, mine, along, src, dst, ssem, rsem, ssem_back, rsem_back):
        half = src.shape[0] // 2
        ahead, back = pl.ds(0, half), pl.ds(half, half)
        sends, receives = copies(count, mine, along, src.at[ahead], dst.at[:, ahead], ssem, rsem)
        sends_back, receives_back = copies(
            count, mine, along, src.at[back], dst.at[:, back], ssem_back, rsem_back
        )

        def start():
            for d in range(1, count):
                sends[d - 1].start()
                pl.when(mine + d >= count)(sends_back[d - 1].start)

        def wait_receives():
            for d in range(1, count):
                receives[d - 1].wait_recv()
                pl.when(mine + d < count)(receives_back[d - 1].wait_recv)

        def wait_sends():
            for d in range(1, count):
                sends[d - 1].wait_send()
                pl.when(mine + d >= count)(sends_back[d - 1].wait_send)

        return start, wait_receives, wait_sends

    def copies(count, mine, along, src, dst, ssem, rsem):
        sends, receives = [], []
        for d in range(1, count):
            where, index = along(d)
            sends.append(
                pltpu.make_async_remote_copy(
                    src_ref=src, dst_ref=dst.at[mine], send_sem=ssem.at[d], recv_sem=rsem.at[mine],
                    device_id=where, device_id_type=pl.DeviceIdType.MESH,
                )
            )
            receives.append(
                pltpu.make_async_remote_copy(
                    src_ref=src, dst_ref=dst.at[index], send_sem=ssem.at[d], recv_sem=rsem.at[index],
                    device_id=where, device_id_type=pl.DeviceIdType.MESH,
                )
            )
        return sends, receives

    x_start, x_wait, x_finish = both_ways(nx, mx, along_x, xsend, xrecv, xs, xr, xs_back, xr_back)
    m_sends, m_receives = copies(ny, my, along_y, msend, mrecv, ms, mr)
    y_start, y_wait, y_finish = both_ways(ny, my, along_y, ysend, yrecv, ys, yr, ys_back, yr_back)
    x_start()

    own_level = lane % levels == sub
    yacc[...] = jnp.zeros_like(yacc)

    def impulse(i):
        return jnp.where(
            (sub < slots) & (sub * LANES + lane >= i * levels) & (sub * LANES + lane < (i + 1) * levels),
            1.0,
            0.0,
        )

    def emit_y(i, states):
        for s in range(slots):
            wt[rows_of(i), s * LANES : (s + 1) * LANES] = jnp.where(
                own_level, spread(states[3][s : s + 1, :]), 0.0
            )
        here = lane_group == lax.rem(i, group)
        chunk = i // group
        for order in range(4):
            yacc[order, chunk] = jnp.where(here, states[order], yacc[order, chunk])

    first, second = sweep(cy, slots, ay, impulse, mid, emit_y)
    packed = pack_maps(first, second, lane_group)
    msend[...] = packed
    mrecv[my] = packed
    for copy in m_sends:
        copy.start()
    y_ends = first + second

    x_wait()
    ends, maps = [], []
    for p in range(nx):
        vectors = [xrecv[p, v] for v in range(4)]
        packed = vectors[0]
        for v, at, row in map_rows(slots):
            packed = jnp.where(sub == row, vectors[v][at : at + 1, :], packed)
        ends.append([open_ends(vectors, k) for k in range(8)])
        maps.append([open_map(packed, k, lane_group, levels) for k in range(8)])
    ahead, behind = compose(nx, mx, slots, lambda p, k: ends[p][k], lambda p, k: maps[p][k])

    def tile(ref, b, s):
        return ref[pl.ds(b * SUB * SUB + s, SUB, stride=SUB), :]

    sums = []
    for b in range(blocks):
        parts = []
        g = [tile(xout, b, slots + 4 - m) for m in range(4)]
        r = [tile(xout, b, slots)] + [tile(xresp.at[2 - m], b, slots) for m in range(3)]
        for s in range(slots):
            value = tile(xout, b, s)
            for m in range(4):
                value = value + g[m] * ahead[m][s : s + 1, :] + r[m] * behind[m][s : s + 1, :]
            grid[b * SUB : (b + 1) * SUB, s * LANES : (s + 1) * LANES] = value
            parts.append(value)
        sums.append(parts)

    merge = jnp.where(
        lax.broadcasted_iota(jnp.int32, (LANES, LANES), 0) % levels
        == lax.broadcasted_iota(jnp.int32, (LANES, LANES), 1) % levels,
        1.0,
        0.0,
    ).astype(jnp.bfloat16)

    def merged(parts):
        rows = jnp.concatenate(parts, axis=0)
        high = rows.astype(jnp.bfloat16)
        low = (rows - high.astype(jnp.float32)).astype(jnp.bfloat16)
        return jnp.dot(high, merge, preferred_element_type=jnp.float32) + jnp.dot(
            low, merge, preferred_element_type=jnp.float32
        )

    products = [
        sum(sums[b][s] * y_ends[k][s : s + 1, :] for s in range(slots))
        for k in range(8)
        for b in range(blocks)
    ]
    totals = merged(products)
    shared = ysend.shape[0] < 8
    for v in range(ysend.shape[0]):
        packed = jnp.zeros((SUB, LANES), jnp.float32)
        for k, base in ((2 * v, 0), (2 * v + 1, group // 2)) if shared else ((v, 0),):
            for b in range(blocks):
                at = (k * blocks + b) * SUB
                packed = jnp.where(lane_group == base + b, totals[at : at + SUB, :], packed)
        ysend[v] = packed
        yrecv[my, v] = packed
    y_start()

    out[...] = lax.dot_general(
        grid[...], wt[...], (((1,), (1,)), ((), ())), precision=HIGHEST, preferred_element_type=jnp.float32
    )

    for copy in m_receives:
        copy.wait_recv()
    maps = [[open_map(mrecv[p], k, lane_group, levels) for k in range(8)] for p in range(ny)]
    y_wait()

    def y_ends_of(p, k):
        if not shared:
            return yrecv[p, k]
        vector = yrecv[p, k // 2]
        return pltpu.roll(vector, LANES // 2, 1) if k % 2 else vector

    ahead, behind = compose(ny, my, slots, y_ends_of, lambda p, k: maps[p][k])
    states = list(ahead) + list(behind)
    masked = [jnp.where(lane_group == b, states[m], 0.0) for m in range(8) for b in range(blocks)]
    opened = merged(masked)
    for s in range(slots):
        held = [yacc[order, s] for order in range(4)]
        answers = [held[3][slots + 4 - m : slots + 5 - m, :] for m in range(4)]
        answers += [held[3 - m][slots : slots + 1, :] for m in range(4)]
        for b in range(blocks):
            value = out[b * SUB : (b + 1) * SUB, s * LANES : (s + 1) * LANES]
            for m in range(8):
                at = (m * blocks + b) * SUB
                value = value + opened[at : at + SUB, :] * answers[m]
            out[b * SUB : (b + 1) * SUB, s * LANES : (s + 1) * LANES] = value
    x_finish()
    y_finish()
    for copy in m_sends:
        copy.wait_send()


def body(nx, ny, field, decay_x, decay_y):
    cx, levels = decay_x.shape
    cy = decay_y.shape[0]
    width = cy * levels
    slots = -(-width // LANES)
    padded = slots * LANES
    if padded != width:
        field = jnp.pad(field, ((0, 0), (0, padded - width)))
    longest = max(cx, cy)
    halves = 4 if 2 * (cx // SUB) * levels <= LANES else 8
    vmem = lambda *shape: pltpu.VMEM(shape, jnp.float32)
    dma = pltpu.SemaphoreType.DMA
    result = pl.pallas_call(
        functools.partial(kernel, nx, ny, cx, cy, slots),
        out_shape=jax.ShapeDtypeStruct((cx, padded), jnp.float32),
        in_specs=[pl.BlockSpec(memory_space=pl.ANY)] * 3,
        out_specs=pl.BlockSpec(memory_space=pltpu.VMEM),
        scratch_shapes=[
            vmem(levels, cx),
            vmem(levels, cy),
            vmem(cx, LANES),
            vmem(cy, LANES),
            vmem(cx, SUB, LANES),
            vmem(longest * SUB, LANES),
            vmem(cx * SUB, LANES),
            vmem(3, cx * SUB, LANES),
            vmem(cx, padded),
            vmem(padded, padded),
            vmem(4, slots, SUB, LANES),
            vmem(4, SUB, LANES),
            vmem(nx, 4, SUB, LANES),
            vmem(SUB, LANES),
            vmem(ny, SUB, LANES),
            vmem(halves, SUB, LANES),
            vmem(ny, halves, SUB, LANES),
            *[dma((count,)) for count in (nx, nx, ny, ny, ny, ny, nx, nx, ny, ny, 2 + slots)],
        ],
        compiler_params=pltpu.CompilerParams(collective_id=0, has_side_effects=True),
    )(field, decay_x.T, decay_y.T)
    return result[:, :width] if padded != width else result


def solution(mesh):
    placed = (P("gx", "gy"), P("gx", None), P("gy", None))
    nx, ny = mesh.shape["gx"], mesh.shape["gy"]
    return jax.shard_map(
        functools.partial(body, nx, ny), mesh=mesh, in_specs=placed, out_specs=P("gx", "gy"), check_vma=False
    )
```

```python
import functools

import jax
import jax.numpy as jnp
from jax import lax
from jax.experimental import pallas as pl
from jax.experimental.pallas import tpu as pltpu
from jax.sharding import PartitionSpec as P

LANES = 128
SUB = 8
HIGHEST = lax.Precision.HIGHEST
UNROLL = 16


def iota(dimension):
    return lax.broadcasted_iota(jnp.int32, (SUB, LANES), dimension)


def rows_of(i):
    return pl.ds(pl.multiple_of(i * SUB, SUB), SUB)


def spread(row):
    return jnp.broadcast_to(row, (SUB, LANES))


def sweep(count, slots, decay, load, mid, emit):
    sub = iota(0)
    zero = jnp.zeros((SUB, LANES), jnp.float32)

    def advance(i, states, value):
        a = decay[pl.ds(i, 1), :]
        g = 1.0 - a
        result = []
        for state in states:
            value = a * state + g * value
            result.append(value)
        return tuple(result)

    def forward(i, states):
        states = advance(i, states, load(i))
        kept = states[3]
        for order in range(3):
            kept = jnp.where(sub == slots + 1 + order, states[order], kept)
        mid[rows_of(i), :] = kept
        return states

    def backward(i, states):
        states = advance(i, states, mid[rows_of(i), :])
        emit(i, states)
        return states

    def chunks(step, states, reverse):
        width = UNROLL if count % UNROLL == 0 else 1

        def chunk(j, states):
            for u in range(width):
                i = j * width + u
                states = step(count - 1 - i if reverse else i, states)
            return states

        return lax.fori_loop(0, count // width, chunk, states)

    one = jnp.where(sub > slots, 1.0, 0.0)
    first = chunks(forward, (one, zero, zero, zero), False)
    one = jnp.where(sub == slots, 1.0, 0.0)
    second = chunks(backward, (one, zero, zero, zero), True)
    return first, second


def pack_maps(first, second, lane_group):
    packed = second[0]
    for k in range(1, 8):
        packed = jnp.where(lane_group == k, (second + first)[k], packed)
    return packed


def open_map(packed, k, lane_group, levels):
    value = jnp.where(lane_group == (k + 4) % 8, packed, 0.0)
    shift = levels
    while shift < LANES:
        value = value + pltpu.roll(value, shift, 1)
        shift *= 2
    return value


def pack_ends(ends, packed, slots):
    sub = iota(0)
    half = SUB // 2
    result = [
        jnp.where(sub < half, ends[2 * v], pltpu.roll(ends[2 * v + 1], half, 0)) for v in range(4)
    ]
    for v, at, row in map_rows(slots):
        result[v] = jnp.where(sub == at, packed[row : row + 1, :], result[v])
    return result


def map_rows(slots):
    half = SUB // 2
    last = half - 1
    return (
        (0, last, slots + 1),
        (1, last, slots),
        (2, last, slots + 2),
        (2, half + last, slots + 3),
        (3, last, slots + 4),
    )


def open_ends(vectors, k):
    vector = vectors[k // 2]
    return pltpu.roll(vector, SUB // 2, 0) if k % 2 else vector


def compose(devices, mine, slots, ends, maps):
    zero = jnp.zeros((SUB, LANES), jnp.float32)
    state = [zero] * 4
    entering = []
    picked = [zero] * 4
    for p in range(devices):
        entering.append(state)
        picked = [jnp.where(mine == p, new, old) for new, old in zip(state, picked)]
        if p == devices - 1:
            break
        r = [maps(p, k)[slots + 1 : slots + 2, :] for k in range(4)]
        state = [
            ends(p, k) + sum(r[k - m] * state[m] for m in range(k + 1)) for k in range(4)
        ]
    ahead = picked
    state = [zero] * 4
    picked = [zero] * 4
    for p in range(devices - 1, -1, -1):
        picked = [jnp.where(mine == p, new, old) for new, old in zip(state, picked)]
        if p == 0:
            break
        back = [maps(p, 4 + k) for k in range(4)]
        r = [back[k][slots : slots + 1, :] for k in range(4)]
        before = entering[p]
        state = [
            ends(p, 4 + k)
            + sum(r[k - m] * state[m] for m in range(k + 1))
            + sum(back[k][slots + 4 - m : slots + 5 - m, :] * before[m] for m in range(4))
            for k in range(4)
        ]
    return ahead, picked


def kernel(
    nx, ny, cx, cy, slots,
    field, decay_x_in, decay_y_in, result,
    out,    decay_x, decay_y, ax, ay, xin, mid, xout, xresp, grid, wt, yacc,
    xsend, xrecv, msend, mrecv, ysend, yrecv,
    xs, xr, ms, mr, ys, yr, xs_back, xr_back, ys_back, yr_back, loaded, stored,
):
    levels = decay_x.shape[0]
    group = LANES // levels
    blocks = cx // SUB
    mx, my = lax.axis_index("gx"), lax.axis_index("gy")
    barrier = pltpu.get_barrier_semaphore()
    for d in range(1, nx):
        pl.semaphore_signal(barrier, inc=1, device_id=(lax.rem(mx + d, nx), my), device_id_type=pl.DeviceIdType.MESH)
    for d in range(1, ny):
        pl.semaphore_signal(barrier, inc=1, device_id=(mx, lax.rem(my + d, ny)), device_id_type=pl.DeviceIdType.MESH)

    loads = [
        pltpu.make_async_copy(decay_x_in, decay_x, loaded.at[0]),
        pltpu.make_async_copy(decay_y_in, decay_y, loaded.at[1]),
    ]
    loads += [
        pltpu.make_async_copy(field.at[:, pl.ds(s * LANES, LANES)], xin.at[:, s], loaded.at[2 + s])
        for s in range(slots)
    ]
    for copy in loads:
        copy.start()

    sub, lane = iota(0), iota(1)
    lane_group = lane // levels
    tiling = jnp.where(
        lax.broadcasted_iota(jnp.int32, (levels, LANES), 1) % levels
        == lax.broadcasted_iota(jnp.int32, (levels, LANES), 0),
        1.0,
        0.0,
    )
    for copy, target, source in ((loads[0], ax, decay_x), (loads[1], ay, decay_y)):
        copy.wait()
        target[...] = lax.dot_general(
            source[...], tiling, (((0,), (0,)), ((), ())), precision=HIGHEST, preferred_element_type=jnp.float32
        )
    for copy in loads[2:]:
        copy.wait()

    def emit_x(i, states):
        xout[rows_of(i), :] = states[3]
        for order in range(3):
            xresp[order, rows_of(i), :] = states[order]

    first, second = sweep(
        cx, slots, ax, lambda i: jnp.where(sub < slots, xin[i], 0.0), mid, emit_x
    )
    packed = pack_maps(first, second, lane_group)
    for v, vector in enumerate(pack_ends(first + second, packed, slots)):
        xsend[v] = vector
        xrecv[mx, v] = vector

    pl.semaphore_wait(barrier, nx + ny - 2)

    def along_x(d):
        return (lax.rem(mx + d, nx), my), lax.rem(mx + d, nx)

    def along_y(d):
        return (mx, lax.rem(my + d, ny)), lax.rem(my + d, ny)

    def both_ways(count, mine, along, src, dst, ssem, rsem, ssem_back, rsem_back):
        half = src.shape[0] // 2
        ahead, back = pl.ds(0, half), pl.ds(half, half)
        sends, receives = copies(count, mine, along, src.at[ahead], dst.at[:, ahead], ssem, rsem)
        sends_back, receives_back = copies(
            count, mine, along, src.at[back], dst.at[:, back], ssem_back, rsem_back
        )

        def start():
            for d in range(1, count):
                sends[d - 1].start()
                pl.when(mine + d >= count)(sends_back[d - 1].start)

        def wait_receives():
            for d in range(1, count):
                receives[d - 1].wait_recv()
                pl.when(mine + d < count)(receives_back[d - 1].wait_recv)

        def wait_sends():
            for d in range(1, count):
                sends[d - 1].wait_send()
                pl.when(mine + d >= count)(sends_back[d - 1].wait_send)

        return start, wait_receives, wait_sends

    def copies(count, mine, along, src, dst, ssem, rsem):
        sends, receives = [], []
        for d in range(1, count):
            where, index = along(d)
            sends.append(
                pltpu.make_async_remote_copy(
                    src_ref=src, dst_ref=dst.at[mine], send_sem=ssem.at[d], recv_sem=rsem.at[mine],
                    device_id=where, device_id_type=pl.DeviceIdType.MESH,
                )
            )
            receives.append(
                pltpu.make_async_remote_copy(
                    src_ref=src, dst_ref=dst.at[index], send_sem=ssem.at[d], recv_sem=rsem.at[index],
                    device_id=where, device_id_type=pl.DeviceIdType.MESH,
                )
            )
        return sends, receives

    x_start, x_wait, x_finish = both_ways(nx, mx, along_x, xsend, xrecv, xs, xr, xs_back, xr_back)
    m_sends, m_receives = copies(ny, my, along_y, msend, mrecv, ms, mr)
    y_start, y_wait, y_finish = both_ways(ny, my, along_y, ysend, yrecv, ys, yr, ys_back, yr_back)
    x_start()

    own_level = lane % levels == sub
    yacc[...] = jnp.zeros_like(yacc)

    def impulse(i):
        return jnp.where(
            (sub < slots) & (sub * LANES + lane >= i * levels) & (sub * LANES + lane < (i + 1) * levels),
            1.0,
            0.0,
        )

    def emit_y(i, states):
        for s in range(slots):
            wt[rows_of(i), s * LANES : (s + 1) * LANES] = jnp.where(
                own_level, spread(states[3][s : s + 1, :]), 0.0
            )
        here = lane_group == lax.rem(i, group)
        chunk = i // group
        for order in range(4):
            yacc[order, chunk] = jnp.where(here, states[order], yacc[order, chunk])

    first, second = sweep(cy, slots, ay, impulse, mid, emit_y)
    packed = pack_maps(first, second, lane_group)
    msend[...] = packed
    mrecv[my] = packed
    for copy in m_sends:
        copy.start()
    y_ends = first + second

    x_wait()
    ends, maps = [], []
    for p in range(nx):
        vectors = [xrecv[p, v] for v in range(4)]
        packed = vectors[0]
        for v, at, row in map_rows(slots):
            packed = jnp.where(sub == row, vectors[v][at : at + 1, :], packed)
        ends.append([open_ends(vectors, k) for k in range(8)])
        maps.append([open_map(packed, k, lane_group, levels) for k in range(8)])
    ahead, behind = compose(nx, mx, slots, lambda p, k: ends[p][k], lambda p, k: maps[p][k])

    def tile(ref, b, s):
        return ref[pl.ds(b * SUB * SUB + s, SUB, stride=SUB), :]

    sums = []
    for b in range(blocks):
        parts = []
        g = [tile(xout, b, slots + 4 - m) for m in range(4)]
        r = [tile(xout, b, slots)] + [tile(xresp.at[2 - m], b, slots) for m in range(3)]
        for s in range(slots):
            value = tile(xout, b, s)
            for m in range(4):
                value = value + g[m] * ahead[m][s : s + 1, :] + r[m] * behind[m][s : s + 1, :]
            grid[b * SUB : (b + 1) * SUB, s * LANES : (s + 1) * LANES] = value
            parts.append(value)
        sums.append(parts)

    merge = jnp.where(
        lax.broadcasted_iota(jnp.int32, (LANES, LANES), 0) % levels
        == lax.broadcasted_iota(jnp.int32, (LANES, LANES), 1) % levels,
        1.0,
        0.0,
    ).astype(jnp.bfloat16)

    def merged(parts):
        rows = jnp.concatenate(parts, axis=0)
        high = rows.astype(jnp.bfloat16)
        low = (rows - high.astype(jnp.float32)).astype(jnp.bfloat16)
        return jnp.dot(high, merge, preferred_element_type=jnp.float32) + jnp.dot(
            low, merge, preferred_element_type=jnp.float32
        )

    products = [
        sum(sums[b][s] * y_ends[k][s : s + 1, :] for s in range(slots))
        for k in range(8)
        for b in range(blocks)
    ]
    totals = merged(products)
    shared = ysend.shape[0] < 8
    for v in range(ysend.shape[0]):
        packed = jnp.zeros((SUB, LANES), jnp.float32)
        for k, base in ((2 * v, 0), (2 * v + 1, group // 2)) if shared else ((v, 0),):
            for b in range(blocks):
                at = (k * blocks + b) * SUB
                packed = jnp.where(lane_group == base + b, totals[at : at + SUB, :], packed)
        ysend[v] = packed
        yrecv[my, v] = packed
    y_start()

    out[...] = lax.dot_general(
        grid[...], wt[...], (((1,), (1,)), ((), ())), precision=HIGHEST, preferred_element_type=jnp.float32
    )

    for copy in m_receives:
        copy.wait_recv()
    maps = [[open_map(mrecv[p], k, lane_group, levels) for k in range(8)] for p in range(ny)]
    y_wait()

    def y_ends_of(p, k):
        if not shared:
            return yrecv[p, k]
        vector = yrecv[p, k // 2]
        return pltpu.roll(vector, LANES // 2, 1) if k % 2 else vector

    ahead, behind = compose(ny, my, slots, y_ends_of, lambda p, k: maps[p][k])
    states = list(ahead) + list(behind)
    masked = [jnp.where(lane_group == b, states[m], 0.0) for m in range(8) for b in range(blocks)]
    opened = merged(masked)
    stores = []
    for s in range(slots):
        held = [yacc[order, s] for order in range(4)]
        answers = [held[3][slots + 4 - m : slots + 5 - m, :] for m in range(4)]
        answers += [held[3 - m][slots : slots + 1, :] for m in range(4)]
        for b in range(blocks):
            value = out[b * SUB : (b + 1) * SUB, s * LANES : (s + 1) * LANES]
            for m in range(8):
                at = (m * blocks + b) * SUB
                value = value + opened[at : at + SUB, :] * answers[m]
            out[b * SUB : (b + 1) * SUB, s * LANES : (s + 1) * LANES] = value
        columns = pl.ds(s * LANES, LANES)
        stores.append(pltpu.make_async_copy(out.at[:, columns], result.at[:, columns], stored.at[s]))
        stores[s].start()
    x_finish()
    y_finish()
    for copy in m_sends:
        copy.wait_send()
    for copy in stores:
        copy.wait()


def body(nx, ny, field, decay_x, decay_y):
    cx, levels = decay_x.shape
    cy = decay_y.shape[0]
    width = cy * levels
    slots = -(-width // LANES)
    padded = slots * LANES
    if padded != width:
        field = jnp.pad(field, ((0, 0), (0, padded - width)))
    longest = max(cx, cy)
    halves = 4 if 2 * (cx // SUB) * levels <= LANES else 8
    vmem = lambda *shape: pltpu.VMEM(shape, jnp.float32)
    dma = pltpu.SemaphoreType.DMA
    result = pl.pallas_call(
        functools.partial(kernel, nx, ny, cx, cy, slots),
        out_shape=jax.ShapeDtypeStruct((cx, padded), jnp.float32),
        in_specs=[pl.BlockSpec(memory_space=pltpu.MemorySpace.HBM)] * 3,
        out_specs=pl.BlockSpec(memory_space=pl.ANY),
        scratch_shapes=[
            vmem(cx, padded),
            vmem(levels, cx),
            vmem(levels, cy),
            vmem(cx, LANES),
            vmem(cy, LANES),
            vmem(cx, SUB, LANES),
            vmem(longest * SUB, LANES),
            vmem(cx * SUB, LANES),
            vmem(3, cx * SUB, LANES),
            vmem(cx, padded),
            vmem(padded, padded),
            vmem(4, slots, SUB, LANES),
            vmem(4, SUB, LANES),
            vmem(nx, 4, SUB, LANES),
            vmem(SUB, LANES),
            vmem(ny, SUB, LANES),
            vmem(halves, SUB, LANES),
            vmem(ny, halves, SUB, LANES),
            *[dma((count,)) for count in (nx, nx, ny, ny, ny, ny, nx, nx, ny, ny, 2 + slots, slots)],
        ],
        compiler_params=pltpu.CompilerParams(collective_id=0, has_side_effects=True, vmem_limit_bytes=24 << 20),
    )(*[pltpu.with_memory_space_constraint(v, pltpu.MemorySpace.HBM) for v in (field, decay_x.T, decay_y.T)])
    return result[:, :width] if padded != width else result


def solution(mesh):
    placed = (P("gx", "gy"), P("gx", None), P("gy", None))
    nx, ny = mesh.shape["gx"], mesh.shape["gy"]
    return jax.shard_map(
        functools.partial(body, nx, ny), mesh=mesh, in_specs=placed, out_specs=P("gx", "gy"), check_vma=False
    )
```
